32 devices in a mesh: mkt: 4 (over z), prod: 2 (over core), draw: 4 (over y, x).
Axes of the slice: x: 2, y: 2, z: 4, core: 2. Of those that a mesh axis runs over, the one named last changes fastest.
Arguments:
- start_utility: float32 [1024, 256], P('mkt', 'prod'), may hold values from -5 to -2
- log_shares: float32 [1024, 256], P('mkt', 'prod'), may hold values from -9 to -5
- characteristics: float32 [1024, 8, 256], P('mkt', None, 'prod'), may hold values from -2.5 to 2.5
- coef_scale: float32 [8], replicated, may hold values from 0.1 to 0.3
- taste_draws: float32 [1024, 8, 2048], P('mkt', None, 'draw'), may hold values from -2.5 to 2.5
Outputs:
- mean_utility: float32 [1024, 256], P('mkt', 'prod')
- step_norms: float32 [2], replicated
The draws below stay inside these ranges and needn't reach their ends.
All inputs are finite; a program needn't handle non-finite values.
Results may differ from the reference program's by a relative error of at most 0.0001.
Values sent between devices are 32-bit elements; how exact they have to be, the bound alone decides.
A program may use at most 64 MiB of HBM per device.

```python
import math
import jax
import jax.numpy as jnp
from jax import lax

J = 256
R = 2048
K = 8
ITERS = 2
M = 1024


def block_levels(stream_key, shape, split, low, high):
    level, own = 1.0, jax.random.fold_in(stream_key, 6)
    for position, shards_of in split:
        draws = jnp.exp(jax.random.uniform(jax.random.fold_in(own, position), (shards_of,), jnp.float32, low / len(split), high / len(split)))
        level = level * jnp.repeat(draws, shape[position] // shards_of).reshape([-1 if axis == position else 1 for axis in range(len(shape))])
    return level


def gaussian(key, dims, width, bound, split=(), kind=jnp.bfloat16):
    level = block_levels(key, dims, split, -0.22, 0.18) if split else 1.0
    drawn = jax.random.normal(key, dims, jnp.float32) * width * level
    return jnp.minimum(jnp.maximum(drawn, -bound), bound).astype(kind)


def setup_inputs(seed: int = 0) -> dict:
    splits = jax.random.split(jax.random.key(seed), 6)
    return {
        "start_utility": jnp.clip(-5.0 + 3.0 * jax.random.uniform(splits[0], (M, J), jnp.float32) ** block_levels(splits[0], (M, J), ((0, 4), (1, 2)), -0.2, 0.2), -5.0, -2.0),
        "log_shares": jnp.clip(-9.0 + 4.0 * jax.random.uniform(splits[1], (M, J), jnp.float32) ** block_levels(splits[1], (M, J), ((0, 4), (1, 2)), -0.2, 0.2), -9.0, -5.0),
        "characteristics": gaussian(splits[2], (M, K, J), 1.0, 2.5, ((0, 4), (2, 2)), jnp.float32),
        "coef_scale": jnp.clip(jnp.exp(jax.random.uniform(splits[3], (K,), jnp.float32, math.log(0.1), math.log(0.3))), 0.1, 0.3),
        "taste_draws": gaussian(splits[4], (M, K, R), 1.0, 2.5, ((0, 4), (2, 4)), jnp.float32),
    }


def reference(start_utility, log_shares, characteristics, coef_scale, taste_draws):
    scaled = taste_draws * coef_scale[None, :, None]
    block_size = math.gcd(M, 16)
    block_count = M // block_size

    def predict(utility):

        def market_block(inputs):
            chars_part, scaled_part, util_part = inputs
            spread = jnp.einsum('mkj,mkr->mjr', chars_part, scaled_part, precision=lax.Precision.HIGHEST)
            weight = jnp.exp(util_part[:, :, None] + spread)
            denominator = 1.0 + lax.optimization_barrier(jnp.sum(weight, axis=1, keepdims=True))
            return lax.optimization_barrier(jnp.sum(weight / denominator, axis=2)) / R
        result = lax.map(market_block, (characteristics.reshape(block_count, block_size, K, J), scaled.reshape(block_count, block_size, K, R), utility.reshape(block_count, block_size, J)))
        return result.reshape(M, J)
    utility = start_utility
    norm_list = []
    for iteration in range(ITERS):
        predicted = predict(utility)
        updated = utility + log_shares - jnp.log(predicted)
        change = updated - utility
        norm_list.append(jnp.sqrt(jnp.mean(change * change) + 1e-06))
        utility = updated
    return (utility, jnp.stack(norm_list))
```

```python
import functools
import math

import jax
import jax.numpy as jnp
from jax import lax
from jax.experimental import pallas as pl
from jax.experimental.pallas import tpu as pltpu
from jax.sharding import PartitionSpec as P

ITERS = 2
UNROLL = 2
LOG2E = math.log2(math.e)
MESH = pl.DeviceIdType.MESH
F32, BF16 = jnp.float32, jnp.bfloat16


def split(x):
    high = x.astype(BF16).astype(F32)
    return high, x - high


def kernel(sizes, chunks, coef, start, shares, chars, tastes, out, norms, util, logs, cbuf, tbuf, pred, square,
           util_sem, char_sem, taste_sem, prod_send, prod_recv, sum_send, sum_recv, fin_local, fin_send, fin_recv,
           sq_send, sq_recv):
    n_mkt, n_prod, n_draw = sizes
    m, p, d = lax.axis_index("mkt"), lax.axis_index("prod"), lax.axis_index("draw")
    markets, coefs, width = chars.shape
    share = markets // n_prod
    rows_of = share // chunks
    products = width * n_prod
    draws = tbuf.shape[2]
    lane = min(draws, 128)

    def local_copies(c):
        rows = pl.ds(p * share + c * rows_of, rows_of)
        here = pl.ds(c * rows_of, rows_of)
        return (
            pltpu.make_async_copy(chars.at[rows], cbuf.at[0, here], char_sem.at[c]),
            pltpu.make_async_copy(tastes.at[rows], tbuf.at[here], taste_sem.at[c]),
        )

    mine = pl.ds(p * share, share)
    util_copies = [
        pltpu.make_async_copy(start.at[mine], util.at[:, pl.ds(0, width)], util_sem.at[0]),
        pltpu.make_async_copy(shares.at[mine], logs.at[:, pl.ds(0, width)], util_sem.at[1]),
    ]
    loads = [local_copies(c) for c in range(chunks)]
    for copy in util_copies:
        copy.start()
    for pair in loads:
        for copy in pair:
            copy.start()

    barrier = pltpu.get_barrier_semaphore()
    n_group = n_mkt * n_prod
    me = m * n_prod + p
    for k in range(1, n_group):
        t = lax.rem(me + k, n_group)
        pl.semaphore_signal(barrier, inc=1, device_id=(t // n_prod, lax.rem(t, n_prod), d), device_id_type=MESH)
    for k in range(1, n_draw):
        pl.semaphore_signal(barrier, inc=1, device_id=(m, p, lax.rem(d + k, n_draw)), device_id_type=MESH)
    pl.semaphore_wait(barrier, n_group - 1 + n_draw - 1)

    util_sends, char_sends = [], [[] for _ in range(chunks)]
    for o in range(1, n_prod):
        q = lax.rem(p + o, n_prod)
        target = (m, q, d)
        theirs = pl.ds(q * share, share)
        for i, (src, dst) in enumerate(((start, util), (shares, logs))):
            util_sends.append(pltpu.make_async_remote_copy(
                src.at[theirs], dst.at[:, pl.ds(o * width, width)],
                prod_send.at[chunks + i, o - 1], prod_recv.at[chunks + i, o - 1], device_id=target, device_id_type=MESH))
        for c in range(chunks):
            char_sends[c].append(pltpu.make_async_remote_copy(
                chars.at[pl.ds(q * share + c * rows_of, rows_of)], cbuf.at[o, pl.ds(c * rows_of, rows_of)],
                prod_send.at[c, o - 1], prod_recv.at[c, o - 1], device_id=target, device_id_type=MESH))
    for copy in util_sends:
        copy.start()
    for group in char_sends:
        for copy in group:
            copy.start()

    row_id = lax.broadcasted_iota(jnp.int32, (coefs, width), 0)
    scale = jnp.zeros((coefs, width), F32)
    for k in range(coefs):
        scale = jnp.where(row_id == k, coef[k], scale)
    scale = scale * LOG2E
    urow = lax.broadcasted_iota(jnp.int32, (8, products), 0)
    ones = jnp.ones((16, 2 * lane), BF16)
    plain = jnp.ones((8, draws), F32)

    def market(step, c, i):
        row = c * rows_of + i
        c_high, c_low = split(jnp.concatenate([cbuf[o, row] * scale for o in range(n_prod)], axis=1))
        s_high, s_low = split(tbuf[row])
        u = jnp.broadcast_to(util[pl.ds(row, 1), :] * LOG2E, (8, products))
        u_high, rest = split(u)
        u_mid, u_low = split(rest)
        u_part = jnp.where(urow == 0, u_high, jnp.where(urow == 1, u_mid, jnp.where(urow == 2, u_low, 0.0)))
        left = jnp.concatenate([c_high, c_low, c_high, u_part], axis=0).astype(BF16)
        right = jnp.concatenate([s_high, s_high, s_low, plain], axis=0).astype(BF16)
        total = jnp.zeros((products, lane), F32)
        block = min(draws, 256)
        for b in range(draws // block):
            power = lax.dot_general(left, right[:, b * block:(b + 1) * block], (((0,), (0,)), ((), ())),
                                    preferred_element_type=F32)
            for a in range(block // lane):
                weight = jnp.exp2(power[:, a * lane:(a + 1) * lane])
                inverse = 1.0 / (1.0 + jnp.sum(weight, axis=0, keepdims=True))
                total = total + weight * inverse
        t_high, t_low = split(total)
        both = jnp.concatenate([t_high.astype(BF16), t_low.astype(BF16)], axis=1)
        summed = lax.dot_general(ones, both, (((1,), (1,)), ((), ())), preferred_element_type=F32)
        pred[step, c, d, pl.ds(i, 1), :] = summed[0:1]

    def predict(step, c):
        def body(i, carry):
            for j in range(UNROLL):
                market(step, c, i * UNROLL + j)
            return carry

        lax.fori_loop(0, rows_of // UNROLL, body, 0)

    def sum_copies(step, c):
        return [pltpu.make_async_remote_copy(
            pred.at[step, c, d], pred.at[step, c, d], sum_send.at[step, c, o - 1], sum_recv.at[step, c, o - 1],
            device_id=(m, p, lax.rem(d + o, n_draw)), device_id_type=MESH) for o in range(1, n_draw)]

    pending = {}

    def send_sums(step, c):
        pending[step, c] = sum_copies(step, c)
        for copy in pending[step, c]:
            copy.start()

    parts = [jnp.zeros((8, 128), F32) for _ in range(ITERS)]

    def update(step, c):
        for copy in pending[step, c]:
            copy.wait()
        rows = pl.ds(c * rows_of, rows_of)
        total = pred[step, c, 0]
        for s in range(1, n_draw):
            total = total + pred[step, c, s]
        old = util[rows, :]
        new = old + logs[rows, :] - jnp.log(total / (draws * n_draw))
        change = new - old
        util[rows, :] = new
        change = change * change
        for a in range(rows_of // 8):
            for b in range(products // 128):
                parts[step] = parts[step] + change[a * 8:(a + 1) * 8, b * 128:(b + 1) * 128]

    finals = []

    def finish(c):
        here = pl.ds(c * rows_of, rows_of)
        rows = pl.ds(p * share + c * rows_of, rows_of)
        copy = pltpu.make_async_copy(util.at[here, pl.ds(0, width)], out.at[rows], fin_local.at[c])
        copy.start()
        finals.append(copy)
        for o in range(1, n_prod):
            copy = pltpu.make_async_remote_copy(
                util.at[here, pl.ds(o * width, width)], out.at[rows], fin_send.at[c, o - 1], fin_recv.at[c, o - 1],
                device_id=(m, lax.rem(p + n_prod - o, n_prod), d), device_id_type=MESH)
            copy.start()
            finals.append(copy)

    for copy in util_copies + util_sends:
        copy.wait()
    for c in range(chunks):
        for copy in [*loads[c], *char_sends[c]]:
            copy.wait()
        predict(0, c)
        send_sums(0, c)
    for step in range(1, ITERS):
        for c in range(chunks):
            update(step - 1, c)
            predict(step, c)
            send_sums(step, c)
    for c in range(chunks):
        update(ITERS - 1, c)
        finish(c)

    for step in range(ITERS):
        square[me, step] = parts[step]
    copies = []
    for k in range(1, n_group):
        t = lax.rem(me + k, n_group)
        copies.append(pltpu.make_async_remote_copy(
            square.at[me], square.at[me], sq_send.at[k - 1], sq_recv.at[k - 1],
            device_id=(t // n_prod, lax.rem(t, n_prod), d), device_id_type=MESH))
    for copy in copies:
        copy.start()
    for copy in copies:
        copy.wait()
    cells = markets * n_mkt * products
    for step in range(ITERS):
        total = square[0, step]
        for k in range(1, n_group):
            total = total + square[k, step]
        mean = jnp.full((8, 128), jnp.sum(total) / cells + 1e-06, F32)
        norms[step] = jnp.max(jnp.sqrt(mean))
    for copy in finals:
        copy.wait()


def solution(mesh):
    sizes = tuple(mesh.shape[name] for name in ("mkt", "prod", "draw"))
    n_mkt, n_prod, n_draw = sizes

    def shards(start_utility, log_shares, characteristics, coef_scale, taste_draws):
        markets, coefs, width = characteristics.shape
        draws = taste_draws.shape[2]
        share = markets // n_prod
        chunks = math.gcd(share // 8, 4)
        rows_of = share // chunks
        products = width * n_prod
        dma = pltpu.SemaphoreType.DMA
        pairs = n_prod - 1
        anywhere = pl.BlockSpec(memory_space=pl.ANY)
        return pl.pallas_call(
            functools.partial(kernel, sizes, chunks),
            out_shape=(jax.ShapeDtypeStruct((markets, width), F32), jax.ShapeDtypeStruct((ITERS,), F32)),
            in_specs=[pl.BlockSpec(memory_space=pltpu.SMEM)] + [anywhere] * 4,
            out_specs=(anywhere, pl.BlockSpec(memory_space=pltpu.SMEM)),
            scratch_shapes=[
                pltpu.VMEM((share, products), F32),
                pltpu.VMEM((share, products), F32),
                pltpu.VMEM((n_prod, share, coefs, width), F32),
                pltpu.VMEM((share, coefs, draws), F32),
                pltpu.VMEM((ITERS, chunks, n_draw, rows_of, products), F32),
                pltpu.VMEM((n_mkt * n_prod, ITERS, 8, 128), F32),
                dma((2,)), dma((chunks,)), dma((chunks,)),
                dma((chunks + 2, pairs)), dma((chunks + 2, pairs)),
                dma((ITERS, chunks, n_draw - 1)), dma((ITERS, chunks, n_draw - 1)),
                dma((chunks,)), dma((chunks, pairs)), dma((chunks, pairs)),
                dma((n_mkt * n_prod - 1,)), dma((n_mkt * n_prod - 1,)),
            ],
            compiler_params=pltpu.CompilerParams(collective_id=0, has_side_effects=True),
        )(coef_scale, start_utility, log_shares, characteristics, taste_draws)

    return jax.shard_map(
        shards,
        mesh=mesh,
        in_specs=(P("mkt", "prod"), P("mkt", "prod"), P("mkt", None, "prod"), P(), P("mkt", None, "draw")),
        out_specs=(P("mkt", "prod"), P()),
        check_vma=False,
    )
```

```python
import functools
import math

import jax
import jax.numpy as jnp
from jax import lax
from jax.experimental import pallas as pl
from jax.experimental.pallas import tpu as pltpu
from jax.sharding import PartitionSpec as P

ITERS = 2
UNROLL = 8
LOG2E = math.log2(math.e)
MESH = pl.DeviceIdType.MESH
F32, BF16 = jnp.float32, jnp.bfloat16


def split(x):
    high = x.astype(BF16).astype(F32)
    return high, x - high


def kernel(sizes, chunks, coef, start, shares, chars, tastes, out, norms, util, logs, cbuf, tbuf, pred, square, turned,
           util_sem, char_sem, taste_sem, prod_send, prod_recv, sum_send, sum_recv, fin_local, fin_send, fin_recv,
           sq_send, sq_recv):
    n_mkt, n_prod, n_draw = sizes
    m, p, d = lax.axis_index("mkt"), lax.axis_index("prod"), lax.axis_index("draw")
    markets, coefs, width = chars.shape
    share = markets // n_prod
    rows_of = share // chunks
    products = width * n_prod
    draws = tbuf.shape[2]
    lane = min(draws, 128)

    def local_copies(c):
        rows = pl.ds(p * share + c * rows_of, rows_of)
        here = pl.ds(c * rows_of, rows_of)
        return (
            pltpu.make_async_copy(chars.at[rows], cbuf.at[0, here], char_sem.at[c]),
            pltpu.make_async_copy(tastes.at[rows], tbuf.at[here], taste_sem.at[c]),
        )

    mine = pl.ds(p * share, share)
    util_copies = [
        pltpu.make_async_copy(start.at[mine], util.at[:, pl.ds(0, width)], util_sem.at[0]),
        pltpu.make_async_copy(shares.at[mine], logs.at[:, pl.ds(0, width)], util_sem.at[1]),
    ]
    loads = [local_copies(c) for c in range(chunks)]
    for copy in util_copies:
        copy.start()
    for pair in loads:
        for copy in pair:
            copy.start()

    barrier = pltpu.get_barrier_semaphore()
    n_group = n_mkt * n_prod
    me = m * n_prod + p
    for k in range(1, n_group):
        t = lax.rem(me + k, n_group)
        pl.semaphore_signal(barrier, inc=1, device_id=(t // n_prod, lax.rem(t, n_prod), d), device_id_type=MESH)
    for k in range(1, n_draw):
        pl.semaphore_signal(barrier, inc=1, device_id=(m, p, lax.rem(d + k, n_draw)), device_id_type=MESH)
    pl.semaphore_wait(barrier, n_group - 1 + n_draw - 1)

    util_sends, char_sends = [], [[] for _ in range(chunks)]
    for o in range(1, n_prod):
        q = lax.rem(p + o, n_prod)
        target = (m, q, d)
        theirs = pl.ds(q * share, share)
        for i, (src, dst) in enumerate(((start, util), (shares, logs))):
            util_sends.append(pltpu.make_async_remote_copy(
                src.at[theirs], dst.at[:, pl.ds(o * width, width)],
                prod_send.at[chunks + i, o - 1], prod_recv.at[chunks + i, o - 1], device_id=target, device_id_type=MESH))
        for c in range(chunks):
            char_sends[c].append(pltpu.make_async_remote_copy(
                chars.at[pl.ds(q * share + c * rows_of, rows_of)], cbuf.at[o, pl.ds(c * rows_of, rows_of)],
                prod_send.at[c, o - 1], prod_recv.at[c, o - 1], device_id=target, device_id_type=MESH))
    for copy in util_sends:
        copy.start()
    for group in char_sends:
        for copy in group:
            copy.start()

    row_id = lax.broadcasted_iota(jnp.int32, (coefs, width), 0)
    scale = jnp.zeros((coefs, width), F32)
    for k in range(coefs):
        scale = jnp.where(row_id == k, coef[k], scale)
    scale = scale * LOG2E
    urow = lax.broadcasted_iota(jnp.int32, (8, products), 0)
    column = lax.broadcasted_iota(jnp.int32, turned.shape, 1)
    turned[...] = jnp.zeros(turned.shape, F32)
    plain = jnp.ones((8, draws), F32)

    def market(step, c, i):
        row = c * rows_of + i
        c_high, c_low = split(jnp.concatenate([cbuf[o, row] * scale for o in range(n_prod)], axis=1))
        s_high, s_low = split(tbuf[row])
        u = jnp.broadcast_to(util[pl.ds(row, 1), :] * LOG2E, (8, products))
        u_high, rest = split(u)
        u_mid, u_low = split(rest)
        u_part = jnp.where(urow == 0, u_high, jnp.where(urow == 1, u_mid, jnp.where(urow == 2, u_low, 0.0)))
        left = jnp.concatenate([c_high, c_low, c_high, u_part], axis=0).astype(BF16)
        right = jnp.concatenate([s_high, s_high, s_low, plain], axis=0).astype(BF16)
        total = jnp.zeros((products, lane), F32)
        block = min(draws, 256)
        for b in range(draws // block):
            power = lax.dot_general(left, right[:, b * block:(b + 1) * block], (((0,), (0,)), ((), ())),
                                    preferred_element_type=F32)
            for a in range(block // lane):
                weight = jnp.exp2(power[:, a * lane:(a + 1) * lane])
                inverse = 1.0 / (1.0 + jnp.sum(weight, axis=0, keepdims=True))
                total = total + weight * inverse
        return jnp.sum(total, axis=1, keepdims=True)

    def predict(step, c):
        def body(i, carry):
            sums = [market(step, c, i * UNROLL + j) for j in range(UNROLL)]
            held = turned[...]
            for j in range(UNROLL):
                held = jnp.where(column == i * UNROLL + j, sums[j], held)
            turned[...] = held
            return carry

        lax.fori_loop(0, rows_of // UNROLL, body, 0)
        pred[step, c, d] = turned[...].T[0:rows_of]

    def sum_copies(step, c):
        return [pltpu.make_async_remote_copy(
            pred.at[step, c, d], pred.at[step, c, d], sum_send.at[step, c, o - 1], sum_recv.at[step, c, o - 1],
            device_id=(m, p, lax.rem(d + o, n_draw)), device_id_type=MESH) for o in range(1, n_draw)]

    pending = {}

    def send_sums(step, c):
        pending[step, c] = sum_copies(step, c)
        for copy in pending[step, c]:
            copy.start()

    parts = [jnp.zeros((8, 128), F32) for _ in range(ITERS)]

    def update(step, c):
        for copy in pending[step, c]:
            copy.wait()
        rows = pl.ds(c * rows_of, rows_of)
        total = pred[step, c, 0]
        for s in range(1, n_draw):
            total = total + pred[step, c, s]
        old = util[rows, :]
        new = old + logs[rows, :] - jnp.log(total / (draws * n_draw))
        change = new - old
        util[rows, :] = new
        change = change * change
        for a in range(rows_of // 8):
            for b in range(products // 128):
                parts[step] = parts[step] + change[a * 8:(a + 1) * 8, b * 128:(b + 1) * 128]

    finals = []

    def finish(c):
        here = pl.ds(c * rows_of, rows_of)
        rows = pl.ds(p * share + c * rows_of, rows_of)
        copy = pltpu.make_async_copy(util.at[here, pl.ds(0, width)], out.at[rows], fin_local.at[c])
        copy.start()
        finals.append(copy)
        for o in range(1, n_prod):
            copy = pltpu.make_async_remote_copy(
                util.at[here, pl.ds(o * width, width)], out.at[rows], fin_send.at[c, o - 1], fin_recv.at[c, o - 1],
                device_id=(m, lax.rem(p + n_prod - o, n_prod), d), device_id_type=MESH)
            copy.start()
            finals.append(copy)

    for copy in util_copies + util_sends:
        copy.wait()
    for c in range(chunks):
        for copy in [*loads[c], *char_sends[c]]:
            copy.wait()
        predict(0, c)
        send_sums(0, c)
    for step in range(1, ITERS):
        for c in range(chunks):
            update(step - 1, c)
            predict(step, c)
            send_sums(step, c)
    for c in range(chunks):
        update(ITERS - 1, c)
        finish(c)

    for step in range(ITERS):
        square[me, step] = parts[step]
    copies = []
    for k in range(1, n_group):
        t = lax.rem(me + k, n_group)
        copies.append(pltpu.make_async_remote_copy(
            square.at[me], square.at[me], sq_send.at[k - 1], sq_recv.at[k - 1],
            device_id=(t // n_prod, lax.rem(t, n_prod), d), device_id_type=MESH))
    for copy in copies:
        copy.start()
    for copy in copies:
        copy.wait()
    cells = markets * n_mkt * products
    for step in range(ITERS):
        total = square[0, step]
        for k in range(1, n_group):
            total = total + square[k, step]
        mean = jnp.full((8, 128), jnp.sum(total) / cells + 1e-06, F32)
        norms[step] = jnp.max(jnp.sqrt(mean))
    for copy in finals:
        copy.wait()


def solution(mesh):
    sizes = tuple(mesh.shape[name] for name in ("mkt", "prod", "draw"))
    n_mkt, n_prod, n_draw = sizes

    def shards(start_utility, log_shares, characteristics, coef_scale, taste_draws):
        markets, coefs, width = characteristics.shape
        draws = taste_draws.shape[2]
        share = markets // n_prod
        chunks = math.gcd(share // 8, 4)
        rows_of = share // chunks
        products = width * n_prod
        dma = pltpu.SemaphoreType.DMA
        pairs = n_prod - 1
        anywhere = pl.BlockSpec(memory_space=pl.ANY)
        return pl.pallas_call(
            functools.partial(kernel, sizes, chunks),
            out_shape=(jax.ShapeDtypeStruct((markets, width), F32), jax.ShapeDtypeStruct((ITERS,), F32)),
            in_specs=[pl.BlockSpec(memory_space=pltpu.SMEM)] + [anywhere] * 4,
            out_specs=(anywhere, pl.BlockSpec(memory_space=pltpu.SMEM)),
            scratch_shapes=[
                pltpu.VMEM((share, products), F32),
                pltpu.VMEM((share, products), F32),
                pltpu.VMEM((n_prod, share, coefs, width), F32),
                pltpu.VMEM((share, coefs, draws), F32),
                pltpu.VMEM((ITERS, chunks, n_draw, rows_of, products), F32),
                pltpu.VMEM((n_mkt * n_prod, ITERS, 8, 128), F32),
                pltpu.VMEM((products, 128), F32),
                dma((2,)), dma((chunks,)), dma((chunks,)),
                dma((chunks + 2, pairs)), dma((chunks + 2, pairs)),
                dma((ITERS, chunks, n_draw - 1)), dma((ITERS, chunks, n_draw - 1)),
                dma((chunks,)), dma((chunks, pairs)), dma((chunks, pairs)),
                dma((n_mkt * n_prod - 1,)), dma((n_mkt * n_prod - 1,)),
            ],
            compiler_params=pltpu.CompilerParams(collective_id=0, has_side_effects=True),
        )(coef_scale, start_utility, log_shares, characteristics, taste_draws)

    return jax.shard_map(
        shards,
        mesh=mesh,
        in_specs=(P("mkt", "prod"), P("mkt", "prod"), P("mkt", None, "prod"), P(), P("mkt", None, "draw")),
        out_specs=(P("mkt", "prod"), P()),
        check_vma=False,
    )
```
